32 devices in a mesh: row: 16 (over z, y, x), col: 2 (over core).
Axes of the slice: x: 2, y: 2, z: 4, core: 2. Of those that a mesh axis runs over, the one named last changes fastest.
Arguments:
- block_ids: int32 [64, 8], replicated, may hold values from 0 to 383, as said below
- iface_counts: int32 [64], replicated, may hold values from 6 to 8
- inv_factor: bfloat16 [30208, 472], P(('row', 'col')), as said below
- coupling: bfloat16 [30208, 1024], P(('row', 'col')), may hold values from -0.375 to 0.375
- boundary_block: bfloat16 [24, 2048, 8, 256], P(None, 'row', None, 'col'), may hold values from -6 to 6
Outputs:
- schur: float32 [24, 2048, 8, 256], P(None, 'row', None, 'col')
The draws below stay inside these ranges and needn't reach their ends.
Inputs may be any that keep to these rules, and one draw needn't show every extreme that they name: For j < 2, block_ids[s, j] is below 16, equals (s // 2 + j) modulo 2, and is the same for the 2 substructures that share s // 2. Apart from these shared first 2 ids, the ids of the 2 substructures that share s // 2 are distinct modulo 16. `inv_factor`: each substructure's block is lower triangular with a diagonal from 0.5 to 1.5.
All inputs are finite; a program needn't handle non-finite values.
Results may differ from the reference program's by a relative error of at most 0.00044.
Values sent between devices are 32-bit elements; how exact they have to be, the bound alone decides.
A program may use at most 64 MiB of HBM per device.

```python
import jax
import jax.numpy as jnp
from jax import lax

NI = 472
NB = 8
CS = 2
NQ = 24
CB = 16
SD = 2
SUBS = 64
CQ = 8
N_ROW = 16
N_COL = 2


def draw_block_ids(key, part):
    places = N_ROW * N_COL
    member = jnp.arange(places, dtype=jnp.int32) % N_COL
    keys = jax.random.split(jax.random.fold_in(key, 11), 3)
    columns = jnp.stack([(member + j) % N_COL for j in range(CS)], axis=1)
    depth = jax.random.randint(keys[0], (places, CS), 0, CB // N_COL)
    span_ids = columns + N_COL * depth
    used = jnp.any((span_ids % N_ROW)[:, :, None] == jnp.arange(N_ROW, dtype=jnp.int32)[None, None, :], axis=1)
    scores = jax.random.randint(keys[1], (places, N_ROW), 0, 2 ** 20) * N_ROW + jnp.arange(N_ROW, dtype=jnp.int32)[None, :]
    scores = scores + used.astype(jnp.int32) * 2 ** 26
    order = jnp.argsort(scores, axis=1)
    owners = order[:, :SD * (NB - CS)].astype(jnp.int32).reshape(places, SD, NB - CS)
    others = owners + N_ROW * jax.random.randint(keys[2], (places, SD, NB - CS), 0, NQ)
    shared = jnp.broadcast_to(span_ids[:, None, :], (places, SD, CS))
    return jnp.concatenate([shared, others], axis=2).reshape(places * SD, NB).astype(jnp.int32)


def draw_inv_factor(key, part):
    subs = SD * N_ROW * N_COL
    first, second = jax.random.split(jax.random.fold_in(key, 23))
    spread = jax.random.normal(first, (subs, NI, NI), jnp.float32)
    lower = jnp.tril(jnp.ones((NI, NI), jnp.float32), -1)
    pivots = jax.random.uniform(second, (subs, NI), jnp.float32, 0.5, 1.5)
    matrix = spread * lower[None] * NI ** (-0.5) + pivots[:, :, None] * jnp.eye(NI, dtype=jnp.float32)[None]
    return matrix.reshape(subs * NI, NI).astype(jnp.bfloat16)


def plant(drawn, own_key, low, top_value):
    spot = [jax.random.randint(jax.random.fold_in(own_key, axis), (), 0, length) for axis, length in enumerate(drawn.shape)]
    widest = drawn.shape.index(max(drawn.shape))
    neighbour = spot[:widest] + [(spot[widest] + 1) % drawn.shape[widest]] + spot[widest + 1:]
    return drawn.at[tuple(spot)].set(low).at[tuple(neighbour)].set(top_value)


def shard_levels(rng, extent, pieces, least, high):
    factor_of = 1.0
    for position, shards_of in pieces:
        steps = jax.random.uniform(jax.random.fold_in(jax.random.fold_in(rng, 6), position), (shards_of,), jnp.float32, least / len(pieces), high / len(pieces))
        factor_of = factor_of * jnp.repeat(jnp.exp(steps), extent[position] // shards_of).reshape((-1,) + (1,) * (len(extent) - 1 - position))
    return factor_of


def noise(own_key, extent, scale, bound, pieces=(), kind=jnp.bfloat16):
    result = jax.random.normal(own_key, extent, jnp.float32) * scale
    if len(pieces) > 0:
        result = shard_levels(own_key, extent, pieces, -0.22, 0.18) * result
    return jnp.clip(result, min=-bound, max=bound).astype(kind)


def setup_inputs(seed: int = 0) -> dict:
    key_list = jax.random.split(jax.random.key(seed), 6)
    block_ids = draw_block_ids(jax.random.fold_in(key_list[5], 71), 0)
    iface_counts = plant(jax.random.randint(key_list[1], (SUBS,), max(CS, NB - 2), NB + 1), jax.random.fold_in(key_list[1], 1), max(CS, NB - 2), NB).astype(jnp.int32)
    inv_factor = draw_inv_factor(jax.random.fold_in(key_list[5], 71), 0)
    coupling = noise(key_list[3], (SUBS * NI, NB * 128), (NI // 2) ** -0.5, 0.375, ((0, 32),))
    boundary_block = noise(key_list[4], (NQ, N_ROW * 128, CQ, N_COL * 128), 1.0, 6.0, ((1, 16), (3, 2)))
    return {"block_ids": block_ids, "iface_counts": iface_counts, "inv_factor": inv_factor, "coupling": coupling, "boundary_block": boundary_block}


def reference(block_ids, iface_counts, inv_factor, coupling, boundary_block):
    subs = SD * N_ROW * N_COL
    factors = inv_factor.reshape(subs, NI, NI)
    couples = coupling.reshape(subs, NI, NB * 128)
    total = jnp.zeros((NQ * N_ROW, 128, CB, 128), jnp.float32)

    def visit(total, item):
        factor, couple, ids, count = item
        mixed = jnp.dot(factor, couple, preferred_element_type=jnp.float32).astype(jnp.bfloat16)
        partial_value = lax.dot_general(mixed, mixed[:, :CS * 128], (((0,), (0,)), ((), ())), preferred_element_type=jnp.float32)
        live = (jnp.arange(NB, dtype=jnp.int32) < count).astype(jnp.float32)
        tiles = partial_value.reshape(NB, 128, CS, 128) * live[:, None, None, None]
        tiles = tiles.transpose(0, 2, 1, 3)
        total = total.at[ids[:, None], :, ids[None, :CS], :].add(tiles)
        return total, None

    total, unused = lax.scan(visit, total, (factors, couples, block_ids, iface_counts))
    dense = total.reshape(NQ * N_ROW * 128, CB * 128)
    given = boundary_block.astype(jnp.float32).reshape(NQ * N_ROW * 128, CB * 128)
    return (given - dense).reshape(NQ, N_ROW * 128, CB // N_COL, N_COL * 128)
```

```python
import functools

import jax
import jax.numpy as jnp
from jax import lax
from jax.experimental import pallas as pl
from jax.experimental.pallas import tpu as pltpu
from jax.sharding import PartitionSpec as P

CS = 2
MESH = pl.DeviceIdType.MESH


def exchange_kernel(
    rows, cols, members, slots, width, nq, cq,
    ids_ref, counts_ref, w_ref, k_ref,
    recv_ref, place_ref,
    y_ref, p_ref, send_ref, send_sem, recv_sem,
):
    row_at = lax.axis_index("row")
    col_at = lax.axis_index("col")
    half = rows // 2
    side = row_at // half

    barrier = pltpu.get_barrier_semaphore()
    for r in range(1, rows):
        other = lax.rem(row_at + r, rows)
        pl.semaphore_signal(barrier, inc=1, device_id=(other, col_at), device_id_type=MESH)
    for r in range(rows):
        for j in range(1, CS):
            pl.semaphore_signal(
                barrier, inc=1, device_id=(r, lax.rem(col_at + j, cols)), device_id_type=MESH
            )
            if cols > 2:
                pl.semaphore_signal(
                    barrier, inc=1, device_id=(r, lax.rem(col_at + cols - j, cols)),
                    device_id_type=MESH,
                )

    own = (row_at * cols + col_at) * members
    for m in range(members):
        for n in range(0, slots * 128, 256):
            y_ref[m, :, n : n + 256] = jnp.dot(
                w_ref[m], k_ref[m, :, n : n + 256], preferred_element_type=jnp.float32
            ).astype(jnp.bfloat16)
        for n in range(0, slots, 2):
            part = lax.dot_general(
                y_ref[m, :, n * 128 : n * 128 + 256],
                y_ref[m, :, 0 : CS * 128],
                (((0,), (0,)), ((), ())),
                preferred_element_type=jnp.float32,
            )
            for d in range(2):
                for j in range(CS):
                    p_ref[m * slots + n + d, j] = part[
                        d * 128 : (d + 1) * 128, j * 128 : (j + 1) * 128
                    ]

    targets = []
    for i in range(half):
        targets.append((1 - side) * half + lax.rem(row_at + i, half))
        targets.append(side * half + lax.rem(row_at + i + 1, half))

    partners = (rows - 1) + (CS - 1) * rows * (2 if cols > 2 else 1)
    copies = []
    pending = []
    for i, target in enumerate(targets):
        picks = []
        for m in range(members):
            k, weight = jnp.int32(0), jnp.float32(0.0)
            count = counts_ref[own + m]
            for kk in range(slots):
                hit = (lax.rem(ids_ref[kk, own + m], rows) == target) & (kk < count)
                k = jnp.where(hit, jnp.int32(kk), k)
                weight = jnp.where(hit, jnp.float32(1.0), weight)
            picks.append((m * slots + k, weight))
        if i == 1:
            pl.semaphore_wait(barrier, partners)
        for j in range(CS):
            total = p_ref[picks[0][0], j] * picks[0][1]
            for k, weight in picks[1:]:
                total = total + p_ref[k, j] * weight
            send_ref[j * rows + i] = total
            if j == 0 and i == rows - 1:
                pending.append(
                    pltpu.make_async_copy(
                        send_ref.at[j * rows + i], recv_ref.at[j * rows + row_at], recv_sem
                    )
                )
            else:
                copy = pltpu.make_async_remote_copy(
                    src_ref=send_ref.at[j * rows + i],
                    dst_ref=recv_ref.at[j * rows + row_at],
                    send_sem=send_sem,
                    recv_sem=recv_sem,
                    device_id=(target, lax.rem(col_at + j, cols)),
                    device_id_type=MESH,
                )
                pending.append(copy)
        if i >= 1:
            while len(pending) > CS:
                pending.pop(0).start()
    while pending:
        pending.pop(0).start()

    wide = place_ref.shape[1]
    sources = CS * rows
    cell_iota = lax.broadcasted_iota(jnp.int32, (nq * cq, wide), 0)
    lane_iota = lax.broadcasted_iota(jnp.int32, (nq * cq, wide), 1)

    def add_source(r, cells):
        for j in range(CS):
            first = (r * cols + lax.rem(col_at + cols - j, cols)) * members
            cell = jnp.int32(-1)
            column = lax.div(ids_ref[j, first], cols)
            for m in range(members):
                for kk in range(slots):
                    if m > 0 and kk < CS:
                        continue
                    ident = ids_ref[kk, first + m]
                    cell = jnp.where(
                        lax.rem(ident, rows) == row_at,
                        lax.div(ident, rows) * cq + column,
                        cell,
                    )
            lane = lane_iota - (j * rows + r)
            cells = jnp.where((lane == 0) | (lane == sources), cell, cells)
        return cells

    cells = lax.fori_loop(0, rows, add_source, jnp.full((nq * cq, wide), -1, jnp.int32))
    place_ref[...] = (cells == cell_iota).astype(jnp.float32).astype(jnp.bfloat16)

    pltpu.make_async_copy(recv_ref, recv_ref, recv_sem).wait()
    sent = send_ref.at[pl.ds(0, CS * rows - 1)]
    pltpu.make_async_copy(sent, sent, send_sem).wait()


def place_kernel(sources, place_ref, recv_ref, boundary_ref, out_ref):
    place = place_ref[...]
    nq, height, cq, _ = out_ref.shape
    for a in range(height):
        tile_rows = recv_ref[:, a, :]
        high = tile_rows.astype(jnp.bfloat16)
        low = (tile_rows - high.astype(jnp.float32)).astype(jnp.bfloat16)
        both = jnp.concatenate([high, low], axis=0)
        total = jnp.dot(place, both, preferred_element_type=jnp.float32)
        out_ref[:, a] = boundary_ref[:, a].astype(jnp.float32) - total.reshape(nq, cq, 128)


def on_device(rows, cols, block_ids, iface_counts, inv_factor, coupling, boundary_block):
    slots = block_ids.shape[1]
    width = inv_factor.shape[1]
    members = inv_factor.shape[0] // width
    nq, tall, cq, _ = boundary_block.shape
    sources = CS * rows
    received, place = pl.pallas_call(
        functools.partial(exchange_kernel, rows, cols, members, slots, width, nq, cq),
        out_shape=(
            jax.ShapeDtypeStruct((sources, 128, 128), jnp.float32),
            jax.ShapeDtypeStruct((nq * cq, 2 * sources), jnp.bfloat16),
        ),
        in_specs=[
            pl.BlockSpec(memory_space=pltpu.SMEM),
            pl.BlockSpec(memory_space=pltpu.SMEM),
            pl.BlockSpec(memory_space=pltpu.VMEM),
            pl.BlockSpec(memory_space=pltpu.VMEM),
        ],
        out_specs=(
            pl.BlockSpec(memory_space=pl.ANY),
            pl.BlockSpec(memory_space=pltpu.VMEM),
        ),
        scratch_shapes=[
            pltpu.VMEM((members, width, slots * 128), jnp.bfloat16),
            pltpu.VMEM((members * slots, CS, 128, 128), jnp.float32),
            pltpu.VMEM((sources, 128, 128), jnp.float32),
            pltpu.SemaphoreType.DMA,
            pltpu.SemaphoreType.DMA,
        ],
        compiler_params=pltpu.CompilerParams(collective_id=0, has_side_effects=True),
        name="exchange",
    )(
        block_ids.T,
        iface_counts,
        inv_factor.reshape(members, width, width),
        coupling.reshape(members, width, slots * 128),
    )
    step = 16
    return pl.pallas_call(
        functools.partial(place_kernel, sources),
        grid=(tall // step,),
        out_shape=jax.ShapeDtypeStruct(boundary_block.shape, jnp.float32),
        in_specs=[
            pl.BlockSpec((nq * cq, 2 * sources), lambda i: (0, 0)),
            pl.BlockSpec((sources, step, 128), lambda i: (0, i, 0)),
            pl.BlockSpec((nq, step, cq, 128), lambda i: (0, i, 0, 0)),
        ],
        out_specs=pl.BlockSpec((nq, step, cq, 128), lambda i: (0, i, 0, 0)),
        name="placing",
    )(place, received, boundary_block)


def solution(mesh):
    return jax.shard_map(
        functools.partial(on_device, mesh.shape["row"], mesh.shape["col"]),
        mesh=mesh,
        in_specs=(
            P(),
            P(),
            P(("row", "col"), None),
            P(("row", "col"), None),
            P(None, "row", None, "col"),
        ),
        out_specs=P(None, "row", None, "col"),
        check_vma=False,
    )
```

```python
import functools

import jax
import jax.numpy as jnp
from jax import lax
from jax.experimental import pallas as pl
from jax.experimental.pallas import tpu as pltpu
from jax.sharding import PartitionSpec as P

CS = 2
MESH = pl.DeviceIdType.MESH


def exchange_kernel(
    rows, cols, members, slots, width, nq, cq,
    pieces,
    ids_ref, counts_ref, factor_ref, couple_ref, boundary_ref,
    out_ref,
    w_ref, k_ref, y_ref, p_ref, send_ref, recv_ref, given_ref, place_ref,
    load_sem, send_sem, recv_sem, given_sem,
):
    row_at = lax.axis_index("row")
    col_at = lax.axis_index("col")
    half = rows // 2
    side = row_at // half

    loads = []
    for m in range(members):
        loads.append(
            (
                pltpu.make_async_copy(factor_ref.at[m], w_ref.at[m], load_sem.at[2 * m]),
                pltpu.make_async_copy(couple_ref.at[m], k_ref.at[m], load_sem.at[2 * m + 1]),
            )
        )
        for load in loads[-1]:
            load.start()

    barrier = pltpu.get_barrier_semaphore()
    for r in range(1, rows):
        other = lax.rem(row_at + r, rows)
        pl.semaphore_signal(barrier, inc=1, device_id=(other, col_at), device_id_type=MESH)
    for r in range(rows):
        for j in range(1, CS):
            pl.semaphore_signal(
                barrier, inc=1, device_id=(r, lax.rem(col_at + j, cols)), device_id_type=MESH
            )
            if cols > 2:
                pl.semaphore_signal(
                    barrier, inc=1, device_id=(r, lax.rem(col_at + cols - j, cols)),
                    device_id_type=MESH,
                )

    given = pltpu.make_async_copy(boundary_ref, given_ref, given_sem)
    given.start()

    own = (row_at * cols + col_at) * members
    for m in range(members):
        for load in loads[m]:
            load.wait()
        for n in range(0, slots * 128, 256):
            y_ref[m, :, n : n + 256] = jnp.dot(
                w_ref[m], k_ref[m, :, n : n + 256], preferred_element_type=jnp.float32
            ).astype(jnp.bfloat16)
        for n in range(0, slots, 2):
            part = lax.dot_general(
                y_ref[m, :, n * 128 : n * 128 + 256],
                y_ref[m, :, 0 : CS * 128],
                (((0,), (0,)), ((), ())),
                preferred_element_type=jnp.float32,
            )
            for d in range(2):
                for j in range(CS):
                    p_ref[m * slots + n + d, j] = part[
                        d * 128 : (d + 1) * 128, j * 128 : (j + 1) * 128
                    ]

    targets = []
    for i in range(half):
        targets.append((1 - side) * half + lax.rem(row_at + i, half))
        targets.append(side * half + lax.rem(row_at + i + 1, half))

    partners = (rows - 1) + (CS - 1) * rows * (2 if cols > 2 else 1)
    def route(i, target, j, piece):
        start, height = pieces[piece]
        src = send_ref.at[pl.ds((j * rows + i) * 128 + start, height)]
        dst = recv_ref.at[pl.ds((j * rows + row_at) * 128 + start, height)]
        if j == 0 and i == rows - 1:
            return pltpu.make_async_copy(src, dst, recv_sem.at[piece])
        return pltpu.make_async_remote_copy(
            src_ref=src,
            dst_ref=dst,
            send_sem=send_sem,
            recv_sem=recv_sem.at[piece],
            device_id=(target, lax.rem(col_at + j, cols)),
            device_id_type=MESH,
        )

    for i, target in enumerate(targets):
        picks = []
        for m in range(members):
            k, weight = jnp.int32(0), jnp.float32(0.0)
            count = counts_ref[own + m]
            for kk in range(slots):
                hit = (lax.rem(ids_ref[kk, own + m], rows) == target) & (kk < count)
                k = jnp.where(hit, jnp.int32(kk), k)
                weight = jnp.where(hit, jnp.float32(1.0), weight)
            picks.append((m * slots + k, weight))
        for j in range(CS):
            total = p_ref[picks[0][0], j] * picks[0][1]
            for k, weight in picks[1:]:
                total = total + p_ref[k, j] * weight
            send_ref[(j * rows + i) * 128 : (j * rows + i + 1) * 128] = total
        if i == 1:
            pl.semaphore_wait(barrier, partners)
        if i >= 1:
            for j in range(CS):
                route(i - 1, targets[i - 1], j, 0).start()
    for j in range(CS):
        route(rows - 1, targets[-1], j, 0).start()
    for piece in range(1, len(pieces)):
        for i, target in enumerate(targets):
            for j in range(CS):
                route(i, target, j, piece).start()

    wide = place_ref.shape[1]
    sources = CS * rows
    cell_iota = lax.broadcasted_iota(jnp.int32, (nq * cq, wide), 0)
    lane_iota = lax.broadcasted_iota(jnp.int32, (nq * cq, wide), 1)

    def add_source(r, cells):
        for j in range(CS):
            first = (r * cols + lax.rem(col_at + cols - j, cols)) * members
            cell = jnp.int32(-1)
            column = lax.div(ids_ref[j, first], cols)
            for m in range(members):
                for kk in range(slots):
                    if m > 0 and kk < CS:
                        continue
                    ident = ids_ref[kk, first + m]
                    cell = jnp.where(
                        lax.rem(ident, rows) == row_at,
                        lax.div(ident, rows) * cq + column,
                        cell,
                    )
            lane = lane_iota - (j * rows + r)
            cells = jnp.where((lane == 0) | (lane == sources), cell, cells)
        return cells

    cells = lax.fori_loop(0, rows, add_source, jnp.full((nq * cq, wide), -1, jnp.int32))
    place_ref[...] = (cells == cell_iota).astype(jnp.float32).astype(jnp.bfloat16)

    given.wait()
    place = place_ref[...]
    for piece, (start, height) in enumerate(pieces):
        arrived = recv_ref.at[pl.ds(0, sources * height)]
        pltpu.make_async_copy(arrived, arrived, recv_sem.at[piece]).wait()

        def place_rows(step, carry):
            halves = []
            first = start + step * 4
            for a in range(4):
                line = recv_ref[pl.ds(first + a, sources, stride=128), :]
                high = line.astype(jnp.bfloat16)
                low = (line - high.astype(jnp.float32)).astype(jnp.bfloat16)
                halves.append(jnp.concatenate([high, low], axis=0))
            for a in range(0, 4, 2):
                both = jnp.concatenate(halves[a : a + 2], axis=1)
                total = jnp.dot(place, both, preferred_element_type=jnp.float32)
                for d in range(2):
                    out_ref[:, first + a + d] = given_ref[:, first + a + d].astype(
                        jnp.float32
                    ) - total[:, d * 128 : (d + 1) * 128].reshape(nq, cq, 128)
            return carry

        lax.fori_loop(0, height // 4, place_rows, 0)
    sent = send_ref.at[pl.ds(0, (sources - 1) * 128)]
    pltpu.make_async_copy(sent, sent, send_sem).wait()


def write_kernel(result_ref, out_ref, sem):
    copies = []
    count = 8
    height = result_ref.shape[0] // count
    for i in range(count):
        part = pl.ds(i * height, height)
        copies.append(pltpu.make_async_copy(result_ref.at[part], out_ref.at[part], sem))
        copies[-1].start()
    pltpu.make_async_copy(result_ref, out_ref, sem).wait()


def kept(value):
    return pltpu.with_memory_space_constraint(value, pltpu.HBM)


def on_device(rows, cols, block_ids, iface_counts, inv_factor, coupling, boundary_block):
    slots = block_ids.shape[1]
    width = inv_factor.shape[1]
    members = inv_factor.shape[0] // width
    nq, tall, cq, _ = boundary_block.shape
    sources = CS * rows
    pieces = ((0, 96), (96, 32))
    result = pl.pallas_call(
        functools.partial(exchange_kernel, rows, cols, members, slots, width, nq, cq, pieces),
        out_shape=jax.ShapeDtypeStruct(boundary_block.shape, jnp.float32),
        in_specs=[
            pl.BlockSpec(memory_space=pltpu.SMEM),
            pl.BlockSpec(memory_space=pltpu.SMEM),
            pl.BlockSpec(memory_space=pltpu.HBM),
            pl.BlockSpec(memory_space=pltpu.HBM),
            pl.BlockSpec(memory_space=pltpu.HBM),
        ],
        out_specs=pl.BlockSpec(memory_space=pltpu.VMEM),
        scratch_shapes=[
            pltpu.VMEM((members, width, width), jnp.bfloat16),
            pltpu.VMEM((members, width, slots * 128), jnp.bfloat16),
            pltpu.VMEM((members, width, slots * 128), jnp.bfloat16),
            pltpu.VMEM((members * slots, CS, 128, 128), jnp.float32),
            pltpu.VMEM((sources * 128, 128), jnp.float32),
            pltpu.VMEM((sources * 128, 128), jnp.float32),
            pltpu.VMEM(boundary_block.shape, jnp.bfloat16),
            pltpu.VMEM((nq * cq, 2 * sources), jnp.bfloat16),
            pltpu.SemaphoreType.DMA((2 * members,)),
            pltpu.SemaphoreType.DMA,
            pltpu.SemaphoreType.DMA((len(pieces),)),
            pltpu.SemaphoreType.DMA,
        ],
        compiler_params=pltpu.CompilerParams(
            collective_id=0, has_side_effects=True, vmem_limit_bytes=32 * 1024 * 1024
        ),
        name="exchange",
    )(
        kept(block_ids.T),
        kept(iface_counts),
        kept(inv_factor.reshape(members, width, width)),
        kept(coupling.reshape(members, width, slots * 128)),
        kept(boundary_block),
    )
    return pl.pallas_call(
        write_kernel,
        out_shape=jax.ShapeDtypeStruct(boundary_block.shape, jnp.float32),
        in_specs=[pl.BlockSpec(memory_space=pltpu.VMEM)],
        out_specs=pl.BlockSpec(memory_space=pltpu.HBM),
        scratch_shapes=[pltpu.SemaphoreType.DMA],
        compiler_params=pltpu.CompilerParams(vmem_limit_bytes=16 * 1024 * 1024),
        name="writing",
    )(result)


def solution(mesh):
    return jax.shard_map(
        functools.partial(on_device, mesh.shape["row"], mesh.shape["col"]),
        mesh=mesh,
        in_specs=(
            P(),
            P(),
            P(("row", "col"), None),
            P(("row", "col"), None),
            P(None, "row", None, "col"),
        ),
        out_specs=P(None, "row", None, "col"),
        check_vma=False,
    )
```

```python
import functools

import jax
import jax.numpy as jnp
from jax import lax
from jax.experimental import pallas as pl
from jax.experimental.pallas import tpu as pltpu
from jax.sharding import PartitionSpec as P

CS = 2
MESH = pl.DeviceIdType.MESH


def exchange_kernel(
    rows, cols, members, slots, width, nq, cq,
    pieces,
    ids_ref, counts_ref, factor_ref, couple_ref, boundary_ref,
    out_ref,
    w_ref, k_ref, y_ref, p_ref, send_ref, recv_ref, given_ref, place_ref,
    load_sem, send_sem, recv_sem, given_sem,
):
    row_at = lax.axis_index("row")
    col_at = lax.axis_index("col")
    half = rows // 2
    side = row_at // half

    loads = []
    for m in range(members):
        loads.append(
            (
                pltpu.make_async_copy(factor_ref.at[m], w_ref.at[m], load_sem.at[2 * m]),
                pltpu.make_async_copy(couple_ref.at[m], k_ref.at[m], load_sem.at[2 * m + 1]),
            )
        )
        for load in loads[-1]:
            load.start()

    barrier = pltpu.get_barrier_semaphore()
    for r in range(1, rows):
        other = lax.rem(row_at + r, rows)
        pl.semaphore_signal(barrier, inc=1, device_id=(other, col_at), device_id_type=MESH)
    for r in range(rows):
        for j in range(1, CS):
            pl.semaphore_signal(
                barrier, inc=1, device_id=(r, lax.rem(col_at + j, cols)), device_id_type=MESH
            )
            if cols > 2:
                pl.semaphore_signal(
                    barrier, inc=1, device_id=(r, lax.rem(col_at + cols - j, cols)),
                    device_id_type=MESH,
                )

    given = pltpu.make_async_copy(boundary_ref, given_ref, given_sem)
    given.start()

    split = width // 2 // 128 * 128 + 128
    own = (row_at * cols + col_at) * members
    for m in range(members):
        for load in loads[m]:
            load.wait()
        for n in range(0, slots * 128, 256):
            for top, bottom in ((0, split), (split, width)):
                y_ref[m, top:bottom, n : n + 256] = jnp.dot(
                    w_ref[m, top:bottom, 0:bottom],
                    k_ref[m, 0:bottom, n : n + 256],
                    preferred_element_type=jnp.float32,
                ).astype(jnp.bfloat16)
        for n in range(0, slots, 2):
            part = lax.dot_general(
                y_ref[m, :, n * 128 : n * 128 + 256],
                y_ref[m, :, 0 : CS * 128],
                (((0,), (0,)), ((), ())),
                preferred_element_type=jnp.float32,
            )
            for d in range(2):
                for j in range(CS):
                    p_ref[m * slots + n + d, j] = part[
                        d * 128 : (d + 1) * 128, j * 128 : (j + 1) * 128
                    ]

    targets = []
    for i in range(half):
        targets.append((1 - side) * half + lax.rem(row_at + i, half))
        targets.append(side * half + lax.rem(row_at + i + 1, half))

    partners = (rows - 1) + (CS - 1) * rows * (2 if cols > 2 else 1)
    def route(i, target, j, piece):
        start, height = pieces[piece]
        src = send_ref.at[pl.ds((j * rows + i) * 128 + start, height)]
        dst = recv_ref.at[pl.ds((j * rows + row_at) * 128 + start, height)]
        if j == 0 and i == rows - 1:
            return pltpu.make_async_copy(src, dst, recv_sem.at[piece])
        return pltpu.make_async_remote_copy(
            src_ref=src,
            dst_ref=dst,
            send_sem=send_sem,
            recv_sem=recv_sem.at[piece],
            device_id=(target, lax.rem(col_at + j, cols)),
            device_id_type=MESH,
        )

    for i, target in enumerate(targets):
        picks = []
        for m in range(members):
            k, weight = jnp.int32(0), jnp.float32(0.0)
            count = counts_ref[own + m]
            for kk in range(slots):
                hit = (lax.rem(ids_ref[kk, own + m], rows) == target) & (kk < count)
                k = jnp.where(hit, jnp.int32(kk), k)
                weight = jnp.where(hit, jnp.float32(1.0), weight)
            picks.append((m * slots + k, weight))
        for j in range(CS):
            total = p_ref[picks[0][0], j] * picks[0][1]
            for k, weight in picks[1:]:
                total = total + p_ref[k, j] * weight
            send_ref[(j * rows + i) * 128 : (j * rows + i + 1) * 128] = total
        if i == 1:
            pl.semaphore_wait(barrier, partners)
        if i >= 1:
            for j in range(CS):
                route(i - 1, targets[i - 1], j, 0).start()
    for j in range(CS):
        route(rows - 1, targets[-1], j, 0).start()
    for piece in range(1, len(pieces)):
        for i, target in enumerate(targets):
            for j in range(CS):
                route(i, target, j, piece).start()

    wide = place_ref.shape[1]
    sources = CS * rows
    cell_iota = lax.broadcasted_iota(jnp.int32, (nq * cq, wide), 0)
    lane_iota = lax.broadcasted_iota(jnp.int32, (nq * cq, wide), 1)

    def add_source(r, cells):
        for j in range(CS):
            first = (r * cols + lax.rem(col_at + cols - j, cols)) * members
            cell = jnp.int32(-1)
            column = lax.div(ids_ref[j, first], cols)
            for m in range(members):
                for kk in range(slots):
                    if m > 0 and kk < CS:
                        continue
                    ident = ids_ref[kk, first + m]
                    cell = jnp.where(
                        lax.rem(ident, rows) == row_at,
                        lax.div(ident, rows) * cq + column,
                        cell,
                    )
            lane = lane_iota - (j * rows + r)
            cells = jnp.where((lane == 0) | (lane == sources), cell, cells)
        return cells

    cells = lax.fori_loop(0, rows, add_source, jnp.full((nq * cq, wide), -1, jnp.int32))
    place_ref[...] = (cells == cell_iota).astype(jnp.float32).astype(jnp.bfloat16)

    given.wait()
    place = place_ref[...]
    for piece, (start, height) in enumerate(pieces):
        arrived = recv_ref.at[pl.ds(0, sources * height)]
        pltpu.make_async_copy(arrived, arrived, recv_sem.at[piece]).wait()

        def place_rows(step, carry):
            halves = []
            first = start + step * 4
            for a in range(4):
                line = recv_ref[pl.ds(first + a, sources, stride=128), :]
                high = line.astype(jnp.bfloat16)
                low = (line - high.astype(jnp.float32)).astype(jnp.bfloat16)
                halves.append(jnp.concatenate([high, low], axis=0))
            for a in range(0, 4, 2):
                both = jnp.concatenate(halves[a : a + 2], axis=1)
                total = jnp.dot(place, both, preferred_element_type=jnp.float32)
                for d in range(2):
                    out_ref[:, first + a + d] = given_ref[:, first + a + d].astype(
                        jnp.float32
                    ) - total[:, d * 128 : (d + 1) * 128].reshape(nq, cq, 128)
            return carry

        lax.fori_loop(0, height // 4, place_rows, 0)
    sent = send_ref.at[pl.ds(0, (sources - 1) * 128)]
    pltpu.make_async_copy(sent, sent, send_sem).wait()


def write_kernel(result_ref, out_ref, sem):
    copies = []
    count = 8
    height = result_ref.shape[0] // count
    for i in range(count):
        part = pl.ds(i * height, height)
        copies.append(pltpu.make_async_copy(result_ref.at[part], out_ref.at[part], sem))
        copies[-1].start()
    pltpu.make_async_copy(result_ref, out_ref, sem).wait()


def kept(value):
    return pltpu.with_memory_space_constraint(value, pltpu.HBM)


def on_device(rows, cols, block_ids, iface_counts, inv_factor, coupling, boundary_block):
    slots = block_ids.shape[1]
    width = inv_factor.shape[1]
    members = inv_factor.shape[0] // width
    nq, tall, cq, _ = boundary_block.shape
    sources = CS * rows
    pieces = ((0, 112), (112, 16))
    result = pl.pallas_call(
        functools.partial(exchange_kernel, rows, cols, members, slots, width, nq, cq, pieces),
        out_shape=jax.ShapeDtypeStruct(boundary_block.shape, jnp.float32),
        in_specs=[
            pl.BlockSpec(memory_space=pltpu.SMEM),
            pl.BlockSpec(memory_space=pltpu.SMEM),
            pl.BlockSpec(memory_space=pltpu.HBM),
            pl.BlockSpec(memory_space=pltpu.HBM),
            pl.BlockSpec(memory_space=pltpu.HBM),
        ],
        out_specs=pl.BlockSpec(memory_space=pltpu.VMEM),
        scratch_shapes=[
            pltpu.VMEM((members, width, width), jnp.bfloat16),
            pltpu.VMEM((members, width, slots * 128), jnp.bfloat16),
            pltpu.VMEM((members, width, slots * 128), jnp.bfloat16),
            pltpu.VMEM((members * slots, CS, 128, 128), jnp.float32),
            pltpu.VMEM((sources * 128, 128), jnp.float32),
            pltpu.VMEM((sources * 128, 128), jnp.float32),
            pltpu.VMEM(boundary_block.shape, jnp.bfloat16),
            pltpu.VMEM((nq * cq, 2 * sources), jnp.bfloat16),
            pltpu.SemaphoreType.DMA((2 * members,)),
            pltpu.SemaphoreType.DMA,
            pltpu.SemaphoreType.DMA((len(pieces),)),
            pltpu.SemaphoreType.DMA,
        ],
        compiler_params=pltpu.CompilerParams(
            collective_id=0, has_side_effects=True, vmem_limit_bytes=32 * 1024 * 1024
        ),
        name="exchange",
    )(
        kept(block_ids.T),
        kept(iface_counts),
        kept(inv_factor.reshape(members, width, width)),
        kept(coupling.reshape(members, width, slots * 128)),
        kept(boundary_block),
    )
    return pl.pallas_call(
        write_kernel,
        out_shape=jax.ShapeDtypeStruct(boundary_block.shape, jnp.float32),
        in_specs=[pl.BlockSpec(memory_space=pltpu.VMEM)],
        out_specs=pl.BlockSpec(memory_space=pltpu.HBM),
        scratch_shapes=[pltpu.SemaphoreType.DMA],
        compiler_params=pltpu.CompilerParams(vmem_limit_bytes=16 * 1024 * 1024),
        name="writing",
    )(result)


def solution(mesh):
    return jax.shard_map(
        functools.partial(on_device, mesh.shape["row"], mesh.shape["col"]),
        mesh=mesh,
        in_specs=(
            P(),
            P(),
            P(("row", "col"), None),
            P(("row", "col"), None),
            P(None, "row", None, "col"),
        ),
        out_specs=P(None, "row", None, "col"),
        check_vma=False,
    )
```
